32 devices in a mesh: expert: 4 (over x, core), replica: 8 (over z, y).
Axes of the slice: x: 2, y: 2, z: 4, core: 2. Of those that a mesh axis runs over, the one named last changes fastest.
Arguments:
- tokens: bfloat16 [192, 4096], P(('expert', 'replica')), may hold values from -6 to 6
- out_grad: bfloat16 [192, 4096], P(('expert', 'replica')), may hold values from -2.5 to 2.5
- expert_ids: int32 [192, 2], P(('expert', 'replica')), may hold values from 0 to 3, all different within a row; in each aligned block of 6 rows (0 to 5, 6 to 11, ...) at most 4 rows name the same one
- gates: float32 [192, 2], P(('expert', 'replica')), may hold values from 0.1 to 1
- w_gate: bfloat16 [4, 7168, 4096], P('expert', 'replica'), may hold values from -0.09375 to 0.09375
- w_up: bfloat16 [4, 7168, 4096], P('expert', 'replica'), may hold values from -0.09375 to 0.09375
- w_down: bfloat16 [4, 7168, 4096], P('expert', 'replica'), may hold values from -0.0625 to 0.0625
Outputs:
- gate_grad: float32 [192, 2], P(('expert', 'replica'))
- input_grad: bfloat16 [192, 4096], P(('expert', 'replica'))
- grad_gate: bfloat16 [4, 7168, 4096], P('expert', 'replica')
- grad_up: bfloat16 [4, 7168, 4096], P('expert', 'replica')
- grad_down: bfloat16 [4, 7168, 4096], P('expert', 'replica')
The draws below stay inside these ranges and needn't reach their ends.
Inputs may be any that keep to these rules, and one draw needn't show every extreme that they name: `expert_ids`: each row names 2 different experts; among the rows of one device no expert is named more than 4 times.
All inputs are finite; a program needn't handle non-finite values.
Results may differ from the reference program's by a relative error of at most 0.02.
Values may be sent and summed in bfloat16 or wider, within the bound.
A program may use at most 128 MiB of HBM per device.

```python
import math
import jax
import jax.numpy as jnp
import numpy as np
from jax import lax

D = 4096
FF = 7168
TOP = 2
TOK_DEV = 6
EXPERTS = 4
CAP = 4
TOKENS = 192


def block_levels(key, dims, split, least, top_value):
    factor_of, own = 1.0, jax.random.fold_in(key, 6)
    for dim, shards_of in split:
        steps = jnp.exp(jax.random.uniform(jax.random.fold_in(own, dim), (shards_of,), jnp.float32, least / len(split), top_value / len(split)))
        factor_of = factor_of * jnp.repeat(steps, dims[dim] // shards_of).reshape([-1 if axis == dim else 1 for axis in range(len(dims))])
    return factor_of


def routed_block(stream_key, own, number, rows, count, top, bound, lean):
    ranking = jax.random.permutation(stream_key, count)
    crowded, usual = shares(count, rows * top, bound, lean, True), shares(count, rows * top, bound, lean, False)
    places = jnp.arange(count)

    def named(tallies, rotation):
        used = int((tallies > 0).sum())
        fixed = max(1, used // 4)
        passed = fixed + (places - fixed + rotation * (used - fixed)) % max(1, count - fixed)
        return jnp.zeros((count,), jnp.int32).at[ranking[jnp.where(places < fixed, places, passed)]].set(jnp.asarray(tallies, jnp.int32))

    tallies = jnp.where(number % 4 == 0, named(crowded, number // 4), named(usual, number - number // 4 - 1))
    mixed = jax.random.permutation(jax.random.fold_in(own, 3), count)
    source_of, sink = mixed[0:count // 2 * 2:2], mixed[1:count // 2 * 2:2]
    margin = jnp.minimum(tallies[source_of] - 1, bound - tallies[sink]) // 2
    margin = jnp.where((source_of == ranking[0]) | (sink == ranking[0]) | (tallies[sink] == 0), 0, jnp.maximum(margin, 0))
    passed = jax.random.randint(jax.random.fold_in(own, 4), (count // 2,), 0, 1 << 20) % (margin + 1)
    tallies = tallies.at[source_of].add(-passed).at[sink].add(passed)
    labels = jnp.searchsorted(jnp.cumsum(tallies), jnp.arange(rows * top), side="right").astype(jnp.int32)
    listing = labels.reshape(top, rows).T
    listing = listing[jax.random.permutation(jax.random.fold_in(own, 1), rows)]
    rotation = jax.random.randint(jax.random.fold_in(own, 2), (rows, 1), 0, top)
    return jnp.take_along_axis(listing, (jnp.arange(top)[None, :] + rotation) % top, axis=1)


def shares(amount, total, reach, skew, full):
    weights = [(1 << 20) // math.isqrt(grade ** skew) + 1 for grade in range(1, amount + 1)]
    largest = reach if full else min(reach, max(-(-total // amount), total * weights[0] // sum(weights)))
    least = 1 if total - largest >= amount - 1 else 0
    holding, spare = [largest] + [least] * (amount - 1), total - largest - least * (amount - 1)
    while spare > 0:
        candidates = [i for i in range(1, amount) if holding[i] < largest] or [i for i in range(1, amount) if holding[i] < reach]
        whole, left = sum([weights[i] for i in candidates]), spare
        for i in candidates:
            extra = min(reach - holding[i], max(1, left * weights[i] // whole), spare)
            holding[i] = holding[i] + extra
            spare = spare - extra
    return np.array(holding)


def bell_draw(rng, shape, scale, limit, shards=(), kind=jnp.bfloat16):
    drawn = scale * jax.random.normal(rng, shape, jnp.float32)
    if shards:
        drawn = drawn * block_levels(rng, shape, shards, -0.22, 0.18)
    return jnp.clip(drawn, -limit, limit).astype(kind)


def setup_inputs(seed: int = 0) -> dict:
    streams_of = jax.random.split(jax.random.key(seed), 8)
    tokens = bell_draw(streams_of[0], (TOKENS, D), 1.0, 6.0, ((0, 32),))
    out_grad = bell_draw(streams_of[1], (TOKENS, D), 0.3, 2.5, ((0, 32),))
    expert_ids_keys = jax.random.split(jax.random.fold_in(streams_of[2], 1), TOKENS // TOK_DEV)
    expert_ids_turns = jax.random.permutation(jax.random.fold_in(streams_of[2], 3), TOKENS // TOK_DEV)
    expert_ids = jax.vmap(lambda own, number: routed_block(jax.random.fold_in(streams_of[2], 2), own, number, TOK_DEV, EXPERTS, TOP, CAP, 2))(expert_ids_keys, expert_ids_turns).reshape((TOKENS, TOP))
    gates = jnp.clip(0.1 + 0.9 * jax.random.uniform(streams_of[3], (TOKENS, TOP), jnp.float32) ** block_levels(streams_of[3], (TOKENS, TOP), ((0, 32),), -0.2, 0.2), 0.1, 1.0)
    w_gate = bell_draw(streams_of[4], (EXPERTS, FF, D), D ** -0.5, 0.09375, ((0, 4), (1, 8)))
    w_up = bell_draw(streams_of[5], (EXPERTS, FF, D), D ** -0.5, 0.09375, ((0, 4), (1, 8)))
    w_down = bell_draw(streams_of[6], (EXPERTS, FF, D), FF ** -0.5, 0.0625, ((0, 4), (1, 8)))
    return {"tokens": tokens, "out_grad": out_grad, "expert_ids": expert_ids, "gates": gates, "w_gate": w_gate, "w_up": w_up, "w_down": w_down}


def reference(tokens, out_grad, expert_ids, gates, w_gate, w_up, w_down):
    token_count = tokens.shape[0]
    model_width = tokens.shape[1]
    blocks = token_count // TOK_DEV
    per_block = TOK_DEV * TOP
    block_ids = expert_ids.reshape(blocks, per_block)
    sequence_pos = jnp.arange(per_block, dtype=jnp.int32)
    earlier = sequence_pos[None, :] < sequence_pos[:, None]
    same_expert = block_ids[:, :, None] == block_ids[:, None, :]
    slot_rank = jnp.sum(jnp.logical_and(same_expert, earlier[None, :, :]), axis=2).astype(jnp.int32)
    position = (jnp.arange(blocks, dtype=jnp.int32)[:, None] * CAP + slot_rank).reshape(-1)
    expert_flat = block_ids.reshape(-1).astype(jnp.int32)
    token_flat = jnp.repeat(jnp.arange(token_count, dtype=jnp.int32), TOP)
    slot_total = blocks * CAP
    source = jnp.full((EXPERTS, slot_total), token_count, jnp.int32).at[expert_flat, position].set(token_flat)
    slot_gate = jnp.zeros((EXPERTS, slot_total), jnp.float32).at[expert_flat, position].set(gates.reshape(-1).astype(jnp.float32))
    padded_tokens = jnp.concatenate([tokens, jnp.zeros((1, model_width), tokens.dtype)], axis=0)
    padded_grad = jnp.concatenate([out_grad, jnp.zeros((1, model_width), out_grad.dtype)], axis=0)
    contract = (((1,), (1,)), ((), ()))
    leading = (((0,), (0,)), ((), ()))

    def one_expert(expert_index):
        gathered = padded_tokens[source[expert_index]]
        gathered_grad = padded_grad[source[expert_index]]
        gate_weight = w_gate[expert_index]
        up_weight = w_up[expert_index]
        down_weight = w_down[expert_index]
        gate_pre = lax.dot_general(gathered, gate_weight, contract, preferred_element_type=jnp.float32)
        up_pre = lax.dot_general(gathered, up_weight, contract, preferred_element_type=jnp.float32)
        sigmoid_gate = jax.nn.sigmoid(gate_pre)
        active = gate_pre * sigmoid_gate
        hidden = (active * up_pre).astype(jnp.bfloat16)
        expert_out = jnp.dot(hidden, down_weight, preferred_element_type=jnp.float32)
        products = jnp.sum(gathered_grad.astype(jnp.float32) * expert_out, axis=1)
        scaled = (slot_gate[expert_index][:, None] * gathered_grad.astype(jnp.float32)).astype(jnp.bfloat16)
        hidden_grad = lax.dot_general(scaled, down_weight, contract, preferred_element_type=jnp.float32)
        gate_pre_grad = (hidden_grad * up_pre * sigmoid_gate * (1.0 + gate_pre * (1.0 - sigmoid_gate))).astype(jnp.bfloat16)
        up_pre_grad = (hidden_grad * active).astype(jnp.bfloat16)
        grad_down = lax.dot_general(hidden, scaled, leading, preferred_element_type=jnp.float32).astype(jnp.bfloat16)
        grad_gate = lax.dot_general(gate_pre_grad, gathered, leading, preferred_element_type=jnp.float32).astype(jnp.bfloat16)
        grad_up = lax.dot_general(up_pre_grad, gathered, leading, preferred_element_type=jnp.float32).astype(jnp.bfloat16)
        slot_grad = (jnp.dot(gate_pre_grad, gate_weight, preferred_element_type=jnp.float32) + jnp.dot(up_pre_grad, up_weight, preferred_element_type=jnp.float32)).astype(jnp.bfloat16)
        return products, slot_grad, grad_gate, grad_up, grad_down

    products, slot_grad, grad_gate, grad_up, grad_down = lax.map(one_expert, jnp.arange(EXPERTS, dtype=jnp.int32))
    gate_grad = products[expert_flat, position].reshape(token_count, TOP)
    picked = slot_grad[expert_flat, position].astype(jnp.float32).reshape(token_count, TOP, model_width)
    input_grad = jnp.sum(picked, axis=1).astype(jnp.bfloat16)
    return gate_grad, input_grad, grad_gate, grad_up, grad_down
```

```python
import functools

import jax
import jax.numpy as jnp
from jax import lax
from jax.experimental import pallas as pl
from jax.experimental.pallas import tpu as pltpu
from jax.sharding import PartitionSpec as P

MESH = pl.DeviceIdType.MESH
PAD = 8
CORES = 2
CHUNKS = 4
VMEM_LIMIT = 67043328
F32 = jnp.float32
BF16 = jnp.bfloat16
NT = (((1,), (1,)), ((), ()))


def split_replica(count):
    fast = max(n for n in range(1, count + 1) if count % n == 0 and n * n <= count)
    return count // fast, fast


def exchange_kernel(
    owners, slow, fast, capacity, rows, fan_out,
    tok_ref, grad_ref, meta_ref, wg_hbm, wu_hbm, wd_hbm,
    x_ref, scaled_ref, hid_t_ref, gpg_t_ref, upg_t_ref, gate_grad_ref, input_grad_ref,
    wg, wu, wd, tok_all, grad_all, meta_all, gate_pre, up_pre, out_dot, hidden, gpg, upg,
    ypart, yrecv, zpart, zrecv, epart, erecv, vals, vy, vz, ve,
    w_sem, g_send, g_recv, y_send, y_recv, z_send, z_recv, e_send, e_recv, v_send, v_recv,
):
    replicas = slow * fast
    chips = owners // CORES
    me_e, me_r = lax.axis_index("expert"), lax.axis_index("replica")
    me_s, me_f = me_r // fast, me_r % fast
    me_x, me_k = me_e // CORES, me_e % CORES
    width = x_ref.shape[1]
    slots = x_ref.shape[0]
    chunk = width // CHUNKS

    sizes = {"z": slow, "y": fast, "x": chips, "k": CORES}
    place = {"z": me_s, "y": me_f, "x": me_x, "k": me_k}

    def device(pos):
        return (pos["x"] * CORES + pos["k"], pos["z"] * fast + pos["y"])

    def moved(dim, step):
        pos = dict(place)
        pos[dim] = lax.rem(place[dim] + step + sizes[dim], sizes[dim])
        return pos

    loads = []
    for i, (src, dst) in enumerate(((wg_hbm, wg), (wu_hbm, wu), (wd_hbm, wd))):
        loads.append(pltpu.make_async_copy(src, dst, w_sem.at[i]))
        loads[-1].start()

    barrier = pltpu.get_barrier_semaphore()
    peers = [device(moved("z", i)) for i in range(1, slow)]
    peers += [device(moved("y", i)) for i in range(1, fast)]
    peers += [(lax.rem(me_e + i, owners), me_r) for i in range(1, owners)]
    for peer in peers:
        pl.semaphore_signal(barrier, inc=1, device_id=peer, device_id_type=MESH)
    pl.semaphore_wait(barrier, len(peers))

    def origin(offset):
        pos = {d: lax.rem(place[d] - offset.get(d, 0) + sizes[d], sizes[d]) for d in place}
        e, r = device(pos)
        return e * replicas + r

    sent = []

    def forward(which, own, everyone, order, offset, last):
        block = origin(offset)
        for dim in order[last + 1:]:
            for step in range(1, sizes[dim]):
                src = own if not offset else everyone.at[block]
                copy = pltpu.make_async_remote_copy(
                    src_ref=src, dst_ref=everyone.at[block],
                    send_sem=g_send.at[which, counts[which]], recv_sem=g_recv.at[which, block],
                    device_id=device(moved(dim, step)), device_id_type=MESH,
                )
                counts[which] += 1
                copy.start()
                sent.append(copy)

    counts = [0, 0, 0]
    streams = (
        (2, meta_ref, meta_all, "zyxk"),
        (0, tok_ref, tok_all, "zyxk"),
        (1, grad_ref, grad_all, "zxyk"),
    )
    for which, own, everyone, order in streams:
        forward(which, own, everyone, order, {}, -1)
    me = me_e * replicas + me_r
    for which, own, everyone, order in streams:
        everyone[me] = own[...]
    held = {0: [{}], 1: [{}], 2: [{}]}
    for level in range(4):
        fresh = {0: [], 1: [], 2: []}
        for position in range(len(held[0]) * (max(sizes.values()) - 1)):
            for which, own, everyone, order in streams:
                dim = order[level]
                steps = sizes[dim] - 1
                if position >= len(held[which]) * steps:
                    continue
                base = held[which][position // steps]
                offset = dict(base)
                offset[dim] = position % steps + 1
                block = origin(offset)
                pltpu.make_async_remote_copy(
                    src_ref=everyone.at[block], dst_ref=everyone.at[block],
                    send_sem=g_send.at[which, 0], recv_sem=g_recv.at[which, block],
                    device_id=device(moved("k", 1)), device_id_type=MESH,
                ).wait_recv()
                forward(which, own, everyone, order, offset, level)
                fresh[which].append(offset)
        for which in held:
            held[which] = held[which] + fresh[which]

    total = tok_all.shape[0] * PAD
    meta_t = jnp.transpose(meta_all[...].reshape(total, meta_all.shape[2]))
    lane = lax.broadcasted_iota(jnp.int32, meta_t.shape, 0)
    slot_row = jnp.sum(jnp.where(lane == me_e, meta_t, 0.0), axis=0, keepdims=True)
    gate_row = jnp.sum(jnp.where(lane == me_e + owners, meta_t, 0.0), axis=0, keepdims=True)
    slot_ids = lax.broadcasted_iota(jnp.int32, (slots, total), 0).astype(F32)
    pick = slot_ids == slot_row
    slot_gate = jnp.sum(jnp.where(pick, gate_row, 0.0), axis=1, keepdims=True)
    chosen = jnp.where(pick, 1.0, 0.0).astype(BF16)

    piece = 512

    def columns(c):
        return pl.ds(pl.multiple_of(c * piece, piece), piece)

    for load in loads:
        load.wait()

    gate_pre[...] = jnp.zeros_like(gate_pre)
    up_pre[...] = jnp.zeros_like(up_pre)
    out_dot[...] = jnp.zeros_like(out_dot)

    @pl.loop(0, width // piece)
    def _(c):
        cols = columns(c)
        toks = tok_all[:, :, cols].reshape(total, piece)
        x = jnp.dot(chosen, toks, preferred_element_type=F32).astype(BF16)
        x_ref[:, cols] = x
        grads = grad_all[:, :, cols].reshape(total, piece)
        routed = jnp.dot(chosen, grads, preferred_element_type=F32)
        scaled_ref[:, cols] = (slot_gate * routed).astype(BF16)
        gate_pre[...] += lax.dot_general(x, wg[:, cols], NT, preferred_element_type=F32)
        up_pre[...] += lax.dot_general(x, wu[:, cols], NT, preferred_element_type=F32)
        out_dot[...] += lax.dot_general(
            routed.astype(BF16), wd[:, cols], NT, preferred_element_type=F32
        )

    g, u, v = gate_pre[...], up_pre[...], out_dot[...]
    h = slot_gate * v
    sig = jax.nn.sigmoid(g)
    active = g * sig
    hid = (active * u).astype(BF16)
    hidden[...] = hid
    gpg[...] = (h * u * sig * (1.0 + g * (1.0 - sig))).astype(BF16)
    upg[...] = (h * active).astype(BF16)
    value = jnp.sum(hid.astype(F32) * v, axis=1, keepdims=True)

    def send(src, dst, send_sem, recv_sem, target):
        copy = pltpu.make_async_remote_copy(
            src_ref=src, dst_ref=dst, send_sem=send_sem, recv_sem=recv_sem,
            device_id=target, device_id_type=MESH,
        )
        copy.start()
        sent.append(copy)
        return copy

    y_copies, z_copies, e_copies = [], [], []
    y_rows = slow * owners * capacity
    z_rows = owners * capacity
    for j in range(CHUNKS):
        for q in range(chunk // piece):
            cols = pl.ds(j * chunk + q * piece, piece)
            part = jnp.dot(gpg[...], wg[:, cols], preferred_element_type=F32) + jnp.dot(
                upg[...], wu[:, cols], preferred_element_type=F32
            )
            ypart[j, :, :, pl.ds(q * piece, piece)] = part.astype(BF16).reshape(fast, y_rows, piece)
        y_copies.append([
            send(ypart.at[j, lax.rem(me_f + i, fast)], yrecv.at[j, i - 1],
                 y_send.at[j, i - 1], y_recv.at[j, i - 1], device(moved("y", i)))
            for i in range(1, fast)
        ])

    spread = jnp.transpose(jnp.broadcast_to(value, (slots, 128)))
    vals[0] = spread[:PAD]
    vy_copies = [
        send(vals.at[0], vy.at[i - 1], v_send.at[0, i - 1], v_recv.at[0, i - 1], device(moved("y", i)))
        for i in range(1, fast)
    ]
    hid_t_ref[...] = jnp.transpose(hidden[...])
    gpg_t_ref[...] = jnp.transpose(gpg[...])
    upg_t_ref[...] = jnp.transpose(upg[...])

    for j in range(CHUNKS):
        acc = ypart[j, me_f].astype(F32)
        for i in range(1, fast):
            y_copies[j][i - 1].wait_recv()
            acc += yrecv[j, i - 1].astype(F32)
        zpart[j] = acc.astype(BF16).reshape(slow, z_rows, chunk)
        z_copies.append([
            send(zpart.at[j, lax.rem(me_s + i, slow)], zrecv.at[j, i - 1],
                 z_send.at[j, i - 1], z_recv.at[j, i - 1], device(moved("z", i)))
            for i in range(1, slow)
        ])
        if j == 0:
            acc_v = vals[0]
            for i in range(1, fast):
                vy_copies[i - 1].wait_recv()
                acc_v += vy[i - 1]
            vals[1] = acc_v
            vz_copies = [
                send(vals.at[1], vz.at[i - 1], v_send.at[1, i - 1], v_recv.at[1, i - 1],
                     device(moved("z", i)))
                for i in range(1, slow)
            ]

    for j in range(CHUNKS):
        acc = zpart[j, me_s].astype(F32)
        for i in range(1, slow):
            z_copies[j][i - 1].wait_recv()
            acc += zrecv[j, i - 1].astype(F32)
        for e in range(owners):
            epart[j, e] = acc[e * capacity:(e + 1) * capacity].astype(BF16)
        e_copies.append([
            send(epart.at[j, lax.rem(me_e + i, owners)], erecv.at[j, i - 1],
                 e_send.at[j, i - 1], e_recv.at[j, i - 1], (lax.rem(me_e + i, owners), me_r))
            for i in range(1, owners)
        ])
        if j == 0:
            acc_v = vals[1]
            for i in range(1, slow):
                vz_copies[i - 1].wait_recv()
                acc_v += vz[i - 1]
            vals[2] = acc_v
            ve_copies = [
                send(vals.at[2], ve.at[i - 1], v_send.at[2, i - 1], v_recv.at[2, i - 1],
                     (lax.rem(me_e + i, owners), me_r))
                for i in range(1, owners)
            ]

    meta = meta_ref[...]
    meta_lane = lax.broadcasted_iota(jnp.int32, meta.shape, 1)

    def lane_of(index):
        return jnp.sum(jnp.where(meta_lane == index, meta, 0.0), axis=1, keepdims=True)

    base = ((me_f * slow + me_s) * owners) * capacity
    slot_lane = lax.broadcasted_iota(jnp.int32, (PAD, slots), 1).astype(F32)
    ids = [lane_of(2 * owners + k) for k in range(fan_out)]
    grads_k = [jnp.zeros((PAD, 1), F32) for _ in range(fan_out)]
    spots = []
    for i in range(owners):
        e = lax.rem(me_e - i + owners, owners)
        spot = lane_of(e)
        spots.append((e, spot))
        if i:
            ve_copies[i - 1].wait_recv()
        row = vals[2] if i == 0 else ve[i - 1]
        got = jnp.sum(jnp.where(spot == slot_lane, row, 0.0), axis=1, keepdims=True)
        for k in range(fan_out):
            grads_k[k] += jnp.where(ids[k] == e.astype(F32), got, 0.0)
    for k in range(fan_out):
        gate_grad_ref[:, k:k + 1] = grads_k[k][:rows]

    for j in range(CHUNKS):
        acc = jnp.zeros((PAD, chunk), F32)
        for i in range(owners):
            if i:
                e_copies[j][i - 1].wait_recv()
            block = epart[j, me_e] if i == 0 else erecv[j, i - 1]
            block = block.astype(F32)
            rank = spots[i][1] - (base + me_e * capacity).astype(F32)
            for c in range(capacity):
                acc += jnp.where(rank == c, 1.0, 0.0) * block[c:c + 1]
        input_grad_ref[:, j * chunk:(j + 1) * chunk] = acc[:rows].astype(BF16)

    for copy in sent:
        copy.wait_send()


def grads_kernel(hid_t, gpg_t, upg_t, x, scaled, gg, gu, gd):
    gg[...] = jnp.dot(gpg_t[...], x[...], preferred_element_type=F32).astype(BF16)
    gu[...] = jnp.dot(upg_t[...], x[...], preferred_element_type=F32).astype(BF16)
    gd[...] = jnp.dot(hid_t[...], scaled[...], preferred_element_type=F32).astype(BF16)


def on_device(tokens, out_grad, expert_ids, gates, w_gate, w_up, w_down):
    rows, fan_out = expert_ids.shape
    width = tokens.shape[1]
    owners, replicas = lax.axis_size("expert"), lax.axis_size("replica")
    slow, fast = split_replica(replicas)
    capacity = max(2, 4 * rows * fan_out // (3 * owners))
    devices = owners * replicas
    slots = devices * capacity
    units = w_gate.shape[1]
    chips = owners // CORES
    me_e, me_r = lax.axis_index("expert"), lax.axis_index("replica")

    flat = expert_ids.reshape(-1)
    hot = (flat[:, None] == jnp.arange(owners, dtype=jnp.int32)[None, :]).astype(jnp.int32)
    seq = jnp.arange(rows * fan_out, dtype=jnp.int32)
    earlier = (seq[None, :] < seq[:, None]).astype(jnp.int32)
    rank = jnp.sum(earlier[:, :, None] * hot[None, :, :], axis=1)
    base = (((me_r % fast) * slow + me_r // fast) * owners + me_e) * capacity
    spot = jnp.max(jnp.where(hot == 1, rank + base, -1).reshape(rows, fan_out, owners), axis=1)
    gate = jnp.sum(hot.reshape(rows, fan_out, owners).astype(F32) * gates[:, :, None], axis=1)
    meta = jnp.concatenate([spot.astype(F32), gate, expert_ids.astype(F32)], axis=1)
    meta = jnp.pad(meta, ((0, PAD - rows), (0, 128 - meta.shape[1])), constant_values=-1.0)
    pad = ((0, PAD - rows), (0, 0))
    chunk = width // CHUNKS
    vm = pltpu.VMEM
    dma = pltpu.SemaphoreType.DMA
    sh = jax.ShapeDtypeStruct
    vspec = pl.BlockSpec(memory_space=pltpu.VMEM)
    aspec = pl.BlockSpec(memory_space=pl.ANY)
    x, scaled, hid_t, gpg_t, upg_t, gate_grad, input_grad = pl.pallas_call(
        functools.partial(exchange_kernel, owners, slow, fast, capacity, rows, fan_out),
        out_shape=(
            sh((slots, width), BF16), sh((slots, width), BF16),
            sh((units, slots), BF16), sh((units, slots), BF16), sh((units, slots), BF16),
            sh((rows, fan_out), F32), sh((rows, width), BF16),
        ),
        in_specs=[vspec] * 3 + [aspec] * 3,
        out_specs=(vspec,) * 7,
        scratch_shapes=[
            vm((units, width), BF16), vm((units, width), BF16), vm((units, width), BF16),
            vm((devices, PAD, width), BF16), vm((devices, PAD, width), BF16),
            vm((devices, PAD, 128), F32),
            vm((slots, units), F32), vm((slots, units), F32), vm((slots, units), F32),
            vm((slots, units), BF16), vm((slots, units), BF16), vm((slots, units), BF16),
            vm((CHUNKS, fast, slots // fast, chunk), BF16),
            vm((CHUNKS, fast - 1, slots // fast, chunk), BF16),
            vm((CHUNKS, slow, owners * capacity, chunk), BF16),
            vm((CHUNKS, slow - 1, owners * capacity, chunk), BF16),
            vm((CHUNKS, owners, capacity, chunk), BF16),
            vm((CHUNKS, owners - 1, capacity, chunk), BF16),
            vm((3, PAD, slots), F32), vm((fast - 1, PAD, slots), F32),
            vm((slow - 1, PAD, slots), F32), vm((owners - 1, PAD, slots), F32),
            dma((3,)), dma((3, devices)), dma((3, devices)),
            dma((CHUNKS, fast)), dma((CHUNKS, fast)),
            dma((CHUNKS, slow)), dma((CHUNKS, slow)),
            dma((CHUNKS, owners)), dma((CHUNKS, owners)),
            dma((3, max(owners, slow, fast))), dma((3, max(owners, slow, fast))),
        ],
        compiler_params=pltpu.CompilerParams(
            collective_id=0, has_side_effects=True, vmem_limit_bytes=VMEM_LIMIT
        ),
        name="exchange",
    )(jnp.pad(tokens, pad), jnp.pad(out_grad, pad), meta, w_gate[0], w_up[0], w_down[0])

    block = 512
    whole = lambda a: pl.BlockSpec(a.shape, lambda i: (0, 0))
    cols = lambda n: pl.BlockSpec((n, block), lambda i: (0, i))
    gg, gu, gd = pl.pallas_call(
        grads_kernel,
        grid=(width // block,),
        out_shape=(sh((units, width), BF16),) * 3,
        in_specs=[whole(hid_t), whole(gpg_t), whole(upg_t), cols(slots), cols(slots)],
        out_specs=(cols(units),) * 3,
        compiler_params=pltpu.CompilerParams(vmem_limit_bytes=48 * 1024 * 1024),
        name="weight_grads",
    )(hid_t, gpg_t, upg_t, x, scaled)
    return gate_grad, input_grad, gg[None], gu[None], gd[None]


def solution(mesh):
    tok = P(("expert", "replica"), None)
    weight = P("expert", "replica", None)
    return jax.shard_map(
        on_device,
        mesh=mesh,
        in_specs=(tok,) * 4 + (weight,) * 3,
        out_specs=(tok, tok, weight, weight, weight),
        check_vma=False,
    )
```

```python
import functools

import jax
import jax.numpy as jnp
from jax import lax
from jax.experimental import pallas as pl
from jax.experimental.pallas import tpu as pltpu
from jax.sharding import PartitionSpec as P

MESH = pl.DeviceIdType.MESH
PAD = 8
CORES = 2
CHUNKS = 4
VMEM_LIMIT = 67043328
F32 = jnp.float32
BF16 = jnp.bfloat16
NT = (((1,), (1,)), ((), ()))


def split_replica(count):
    fast = max(n for n in range(1, count + 1) if count % n == 0 and n * n <= count)
    return count // fast, fast


def exchange_kernel(
    owners, slow, fast, capacity, rows, fan_out,
    tok_ref, grad_ref, meta_ref, wg_hbm, wu_hbm, wd_hbm,
    x_ref, scaled_ref, hid_t_ref, gpg_t_ref, upg_t_ref, gate_grad_ref, input_grad_ref,
    wg, wu, wd, tok_all, grad_all, meta_all, gate_pre, up_pre, out_dot, hidden, gpg, upg,
    ypart, yrecv, zpart, zrecv, epart, erecv, vals, vy, vz, ve,
    w_sem, g_send, g_recv, y_send, y_recv, z_send, z_recv, e_send, e_recv, v_send, v_recv,
):
    replicas = slow * fast
    chips = owners // CORES
    me_e, me_r = lax.axis_index("expert"), lax.axis_index("replica")
    me_s, me_f = me_r // fast, me_r % fast
    me_x, me_k = me_e // CORES, me_e % CORES
    width = x_ref.shape[1]
    slots = x_ref.shape[0]
    chunk = width // CHUNKS

    sizes = {"z": slow, "y": fast, "x": chips, "k": CORES}
    place = {"z": me_s, "y": me_f, "x": me_x, "k": me_k}

    def device(pos):
        return (pos["x"] * CORES + pos["k"], pos["z"] * fast + pos["y"])

    def moved(dim, step):
        pos = dict(place)
        pos[dim] = lax.rem(place[dim] + step + sizes[dim], sizes[dim])
        return pos

    loads = []
    for i, (src, dst) in enumerate(((wg_hbm, wg), (wu_hbm, wu), (wd_hbm, wd))):
        loads.append(pltpu.make_async_copy(src, dst, w_sem.at[i]))
        loads[-1].start()

    barrier = pltpu.get_barrier_semaphore()
    peers = [device(moved("z", i)) for i in range(1, slow)]
    peers += [device(moved("y", i)) for i in range(1, fast)]
    peers += [(lax.rem(me_e + i, owners), me_r) for i in range(1, owners)]
    for peer in peers:
        pl.semaphore_signal(barrier, inc=1, device_id=peer, device_id_type=MESH)
    pl.semaphore_wait(barrier, len(peers))

    def origin(offset):
        pos = {d: lax.rem(place[d] - offset.get(d, 0) + sizes[d], sizes[d]) for d in place}
        e, r = device(pos)
        return e * replicas + r

    sent = []

    def forward(which, own, everyone, order, offset, last):
        block = origin(offset)
        for dim in order[last + 1:]:
            for step in range(1, sizes[dim]):
                src = own if not offset else everyone.at[block]
                copy = pltpu.make_async_remote_copy(
                    src_ref=src, dst_ref=everyone.at[block],
                    send_sem=g_send.at[which, counts[which]], recv_sem=g_recv.at[which, block],
                    device_id=device(moved(dim, step)), device_id_type=MESH,
                )
                counts[which] += 1
                copy.start()
                sent.append(copy)

    counts = [0, 0, 0]
    streams = (
        (2, meta_ref, meta_all, "zyxk"),
        (0, tok_ref, tok_all, "zyxk"),
        (1, grad_ref, grad_all, "zxyk"),
    )
    for which, own, everyone, order in streams:
        forward(which, own, everyone, order, {}, -1)
    me = me_e * replicas + me_r
    for which, own, everyone, order in streams:
        everyone[me] = own[...]
    held = {0: [{}], 1: [{}], 2: [{}]}
    for level in range(4):
        fresh = {0: [], 1: [], 2: []}
        for position in range(len(held[0]) * (max(sizes.values()) - 1)):
            for which, own, everyone, order in streams:
                dim = order[level]
                steps = sizes[dim] - 1
                if position >= len(held[which]) * steps:
                    continue
                base = held[which][position // steps]
                offset = dict(base)
                offset[dim] = position % steps + 1
                block = origin(offset)
                pltpu.make_async_remote_copy(
                    src_ref=everyone.at[block], dst_ref=everyone.at[block],
                    send_sem=g_send.at[which, 0], recv_sem=g_recv.at[which, block],
                    device_id=device(moved("k", 1)), device_id_type=MESH,
                ).wait_recv()
                forward(which, own, everyone, order, offset, level)
                fresh[which].append(offset)
        for which in held:
            held[which] = held[which] + fresh[which]

    total = tok_all.shape[0] * PAD
    meta_t = jnp.transpose(meta_all[...].reshape(total, meta_all.shape[2]))
    lane = lax.broadcasted_iota(jnp.int32, meta_t.shape, 0)
    slot_row = jnp.sum(jnp.where(lane == me_e, meta_t, 0.0), axis=0, keepdims=True)
    gate_row = jnp.sum(jnp.where(lane == me_e + owners, meta_t, 0.0), axis=0, keepdims=True)
    slot_ids = lax.broadcasted_iota(jnp.int32, (slots, total), 0).astype(F32)
    pick = slot_ids == slot_row
    slot_gate = jnp.sum(jnp.where(pick, gate_row, 0.0), axis=1, keepdims=True)
    chosen = jnp.where(pick, 1.0, 0.0).astype(BF16)

    piece = 512

    def columns(c):
        return pl.ds(pl.multiple_of(c * piece, piece), piece)

    for load in loads:
        load.wait()

    gate_pre[...] = jnp.zeros_like(gate_pre)
    up_pre[...] = jnp.zeros_like(up_pre)
    out_dot[...] = jnp.zeros_like(out_dot)

    @pl.loop(0, width // piece)
    def _(c):
        cols = columns(c)
        toks = tok_all[:, :, cols].reshape(total, piece)
        x = jnp.dot(chosen, toks, preferred_element_type=F32).astype(BF16)
        x_ref[:, cols] = x
        grads = grad_all[:, :, cols].reshape(total, piece)
        routed = jnp.dot(chosen, grads, preferred_element_type=F32)
        scaled_ref[:, cols] = (slot_gate * routed).astype(BF16)
        gate_pre[...] += lax.dot_general(x, wg[:, cols], NT, preferred_element_type=F32)
        up_pre[...] += lax.dot_general(x, wu[:, cols], NT, preferred_element_type=F32)
        out_dot[...] += lax.dot_general(
            routed.astype(BF16), wd[:, cols], NT, preferred_element_type=F32
        )

    g, u, v = gate_pre[...], up_pre[...], out_dot[...]
    h = slot_gate * v
    sig = jax.nn.sigmoid(g)
    active = g * sig
    hid = (active * u).astype(BF16)
    hidden[...] = hid
    gpg[...] = (h * u * sig * (1.0 + g * (1.0 - sig))).astype(BF16)
    upg[...] = (h * active).astype(BF16)
    value = jnp.sum(hid.astype(F32) * v, axis=1, keepdims=True)

    def send(src, dst, send_sem, recv_sem, target):
        copy = pltpu.make_async_remote_copy(
            src_ref=src, dst_ref=dst, send_sem=send_sem, recv_sem=recv_sem,
            device_id=target, device_id_type=MESH,
        )
        copy.start()
        sent.append(copy)
        return copy

    y_copies, z_copies, e_copies = [], [], []
    y_rows = slow * owners * capacity
    z_rows = owners * capacity
    def pass_on(j):
        acc = ypart[j, me_f].astype(F32)
        for i in range(1, fast):
            y_copies[j][i - 1].wait_recv()
            acc += yrecv[j, i - 1].astype(F32)
        zpart[j] = acc.astype(BF16).reshape(slow, z_rows, chunk)
        z_copies.append([
            send(zpart.at[j, lax.rem(me_s + i, slow)], zrecv.at[j, i - 1],
                 z_send.at[j, i - 1], z_recv.at[j, i - 1], device(moved("z", i)))
            for i in range(1, slow)
        ])

    for j in range(CHUNKS):
        for q in range(chunk // piece):
            cols = pl.ds(j * chunk + q * piece, piece)
            part = jnp.dot(gpg[...], wg[:, cols], preferred_element_type=F32) + jnp.dot(
                upg[...], wu[:, cols], preferred_element_type=F32
            )
            ypart[j, :, :, pl.ds(q * piece, piece)] = part.astype(BF16).reshape(fast, y_rows, piece)
        y_copies.append([
            send(ypart.at[j, lax.rem(me_f + i, fast)], yrecv.at[j, i - 1],
                 y_send.at[j, i - 1], y_recv.at[j, i - 1], device(moved("y", i)))
            for i in range(1, fast)
        ])
        if j:
            pass_on(j - 1)

    spread = jnp.transpose(jnp.broadcast_to(value, (slots, 128)))
    vals[0] = spread[:PAD]
    vy_copies = [
        send(vals.at[0], vy.at[i - 1], v_send.at[0, i - 1], v_recv.at[0, i - 1], device(moved("y", i)))
        for i in range(1, fast)
    ]
    hid_t_ref[...] = jnp.transpose(hidden[...])
    gpg_t_ref[...] = jnp.transpose(gpg[...])
    upg_t_ref[...] = jnp.transpose(upg[...])

    pass_on(CHUNKS - 1)
    acc_v = vals[0]
    for i in range(1, fast):
        vy_copies[i - 1].wait_recv()
        acc_v += vy[i - 1]
    vals[1] = acc_v
    vz_copies = [
        send(vals.at[1], vz.at[i - 1], v_send.at[1, i - 1], v_recv.at[1, i - 1],
             device(moved("z", i)))
        for i in range(1, slow)
    ]

    for j in range(CHUNKS):
        acc = zpart[j, me_s].astype(F32)
        for i in range(1, slow):
            z_copies[j][i - 1].wait_recv()
            acc += zrecv[j, i - 1].astype(F32)
        for e in range(owners):
            epart[j, e] = acc[e * capacity:(e + 1) * capacity].astype(BF16)
        e_copies.append([
            send(epart.at[j, lax.rem(me_e + i, owners)], erecv.at[j, i - 1],
                 e_send.at[j, i - 1], e_recv.at[j, i - 1], (lax.rem(me_e + i, owners), me_r))
            for i in range(1, owners)
        ])
        if j == 0:
            acc_v = vals[1]
            for i in range(1, slow):
                vz_copies[i - 1].wait_recv()
                acc_v += vz[i - 1]
            vals[2] = acc_v
            ve_copies = [
                send(vals.at[2], ve.at[i - 1], v_send.at[2, i - 1], v_recv.at[2, i - 1],
                     (lax.rem(me_e + i, owners), me_r))
                for i in range(1, owners)
            ]

    meta = meta_ref[...]
    meta_lane = lax.broadcasted_iota(jnp.int32, meta.shape, 1)

    def lane_of(index):
        return jnp.sum(jnp.where(meta_lane == index, meta, 0.0), axis=1, keepdims=True)

    base = ((me_f * slow + me_s) * owners) * capacity
    slot_lane = lax.broadcasted_iota(jnp.int32, (PAD, slots), 1).astype(F32)
    ids = [lane_of(2 * owners + k) for k in range(fan_out)]
    grads_k = [jnp.zeros((PAD, 1), F32) for _ in range(fan_out)]
    spots = []
    for i in range(owners):
        e = lax.rem(me_e - i + owners, owners)
        spot = lane_of(e)
        spots.append((e, spot))
        if i:
            ve_copies[i - 1].wait_recv()
        row = vals[2] if i == 0 else ve[i - 1]
        got = jnp.sum(jnp.where(spot == slot_lane, row, 0.0), axis=1, keepdims=True)
        for k in range(fan_out):
            grads_k[k] += jnp.where(ids[k] == e.astype(F32), got, 0.0)
    for k in range(fan_out):
        gate_grad_ref[:, k:k + 1] = grads_k[k][:rows]

    for j in range(CHUNKS):
        acc = jnp.zeros((PAD, chunk), F32)
        for i in range(owners):
            if i:
                e_copies[j][i - 1].wait_recv()
            block = epart[j, me_e] if i == 0 else erecv[j, i - 1]
            block = block.astype(F32)
            rank = spots[i][1] - (base + me_e * capacity).astype(F32)
            for c in range(capacity):
                acc += jnp.where(rank == c, 1.0, 0.0) * block[c:c + 1]
        input_grad_ref[:, j * chunk:(j + 1) * chunk] = acc[:rows].astype(BF16)

    for copy in sent:
        copy.wait_send()


def grads_kernel(hid_t, gpg_t, upg_t, x, scaled, gg, gu, gd):
    gg[...] = jnp.dot(gpg_t[...], x[...], preferred_element_type=F32).astype(BF16)
    gu[...] = jnp.dot(upg_t[...], x[...], preferred_element_type=F32).astype(BF16)
    gd[...] = jnp.dot(hid_t[...], scaled[...], preferred_element_type=F32).astype(BF16)


def on_device(tokens, out_grad, expert_ids, gates, w_gate, w_up, w_down):
    rows, fan_out = expert_ids.shape
    width = tokens.shape[1]
    owners, replicas = lax.axis_size("expert"), lax.axis_size("replica")
    slow, fast = split_replica(replicas)
    capacity = max(2, 4 * rows * fan_out // (3 * owners))
    devices = owners * replicas
    slots = devices * capacity
    units = w_gate.shape[1]
    chips = owners // CORES
    me_e, me_r = lax.axis_index("expert"), lax.axis_index("replica")

    flat = expert_ids.reshape(-1)
    hot = (flat[:, None] == jnp.arange(owners, dtype=jnp.int32)[None, :]).astype(jnp.int32)
    seq = jnp.arange(rows * fan_out, dtype=jnp.int32)
    earlier = (seq[None, :] < seq[:, None]).astype(jnp.int32)
    rank = jnp.sum(earlier[:, :, None] * hot[None, :, :], axis=1)
    base = (((me_r % fast) * slow + me_r // fast) * owners + me_e) * capacity
    spot = jnp.max(jnp.where(hot == 1, rank + base, -1).reshape(rows, fan_out, owners), axis=1)
    gate = jnp.sum(hot.reshape(rows, fan_out, owners).astype(F32) * gates[:, :, None], axis=1)
    meta = jnp.concatenate([spot.astype(F32), gate, expert_ids.astype(F32)], axis=1)
    meta = jnp.pad(meta, ((0, PAD - rows), (0, 128 - meta.shape[1])), constant_values=-1.0)
    pad = ((0, PAD - rows), (0, 0))
    chunk = width // CHUNKS
    vm = pltpu.VMEM
    dma = pltpu.SemaphoreType.DMA
    sh = jax.ShapeDtypeStruct
    vspec = pl.BlockSpec(memory_space=pltpu.VMEM)
    aspec = pl.BlockSpec(memory_space=pl.ANY)
    x, scaled, hid_t, gpg_t, upg_t, gate_grad, input_grad = pl.pallas_call(
        functools.partial(exchange_kernel, owners, slow, fast, capacity, rows, fan_out),
        out_shape=(
            sh((slots, width), BF16), sh((slots, width), BF16),
            sh((units, slots), BF16), sh((units, slots), BF16), sh((units, slots), BF16),
            sh((rows, fan_out), F32), sh((rows, width), BF16),
        ),
        in_specs=[vspec] * 3 + [aspec] * 3,
        out_specs=(vspec,) * 7,
        scratch_shapes=[
            vm((units, width), BF16), vm((units, width), BF16), vm((units, width), BF16),
            vm((devices, PAD, width), BF16), vm((devices, PAD, width), BF16),
            vm((devices, PAD, 128), F32),
            vm((slots, units), F32), vm((slots, units), F32), vm((slots, units), F32),
            vm((slots, units), BF16), vm((slots, units), BF16), vm((slots, units), BF16),
            vm((CHUNKS, fast, slots // fast, chunk), BF16),
            vm((CHUNKS, fast - 1, slots // fast, chunk), BF16),
            vm((CHUNKS, slow, owners * capacity, chunk), BF16),
            vm((CHUNKS, slow - 1, owners * capacity, chunk), BF16),
            vm((CHUNKS, owners, capacity, chunk), BF16),
            vm((CHUNKS, owners - 1, capacity, chunk), BF16),
            vm((3, PAD, slots), F32), vm((fast - 1, PAD, slots), F32),
            vm((slow - 1, PAD, slots), F32), vm((owners - 1, PAD, slots), F32),
            dma((3,)), dma((3, devices)), dma((3, devices)),
            dma((CHUNKS, fast)), dma((CHUNKS, fast)),
            dma((CHUNKS, slow)), dma((CHUNKS, slow)),
            dma((CHUNKS, owners)), dma((CHUNKS, owners)),
            dma((3, max(owners, slow, fast))), dma((3, max(owners, slow, fast))),
        ],
        compiler_params=pltpu.CompilerParams(
            collective_id=0, has_side_effects=True, vmem_limit_bytes=VMEM_LIMIT
        ),
        name="exchange",
    )(jnp.pad(tokens, pad), jnp.pad(out_grad, pad), meta, w_gate[0], w_up[0], w_down[0])

    block = 512
    whole = lambda a: pl.BlockSpec(a.shape, lambda i: (0, 0))
    cols = lambda n: pl.BlockSpec((n, block), lambda i: (0, i))
    gg, gu, gd = pl.pallas_call(
        grads_kernel,
        grid=(width // block,),
        out_shape=(sh((units, width), BF16),) * 3,
        in_specs=[whole(hid_t), whole(gpg_t), whole(upg_t), cols(slots), cols(slots)],
        out_specs=(cols(units),) * 3,
        compiler_params=pltpu.CompilerParams(vmem_limit_bytes=VMEM_LIMIT),
        name="weight_grads",
    )(hid_t, gpg_t, upg_t, x, scaled)
    return gate_grad, input_grad, gg[None], gu[None], gd[None]


def solution(mesh):
    tok = P(("expert", "replica"), None)
    weight = P("expert", "replica", None)
    return jax.shard_map(
        on_device,
        mesh=mesh,
        in_specs=(tok,) * 4 + (weight,) * 3,
        out_specs=(tok, tok, weight, weight, weight),
        check_vma=False,
    )
```
